32 devices in a mesh: dp: 4 (over y, x), tensor: 8 (over z, core).
Axes of the slice: x: 2, y: 2, z: 4, core: 2. Of those that a mesh axis runs over, the one named last changes fastest.
Arguments:
- grad_out: bfloat16 [4096, 8192], P(('dp', 'tensor')), may hold values from -6 to 6
- out_weight: bfloat16 [8192, 4096], P('dp', 'tensor'), may hold values from -0.0625 to 0.0625
- query: bfloat16 [4096, 4096], P('dp', 'tensor'), may hold values from -6 to 6, as said below
- keys: bfloat16 [4096, 256], P('dp'), may hold values from -6 to 6
- values: bfloat16 [4096, 256], P('dp'), may hold values from -6 to 6
- attended: bfloat16 [4096, 4096], P('dp', 'tensor'), may hold values from -6 to 6, as said below
- stats: float32 [32, 4096], P('tensor', 'dp'), as said below
Outputs:
- query_grad: bfloat16 [4096, 4096], P('dp', 'tensor')
- key_grad: bfloat16 [4096, 256], P('dp', 'tensor')
- value_grad: bfloat16 [4096, 256], P('dp', 'tensor')
- weight_grad: bfloat16 [8192, 4096], P('dp', 'tensor')
The draws below stay inside these ranges and needn't reach their ends.
Inputs may be any that keep to these rules, and one draw needn't show every extreme that they name: query, keys and values are independent draws. attended is the causal attention output of the given query, keys and values within each sequence of 1024 rows: query head h uses key head h // 16, scores scaled by 128 ** -0.5, softmax over keys at or before the query. stats[h, t] is the logarithm of the sum of exp(score) over the keys that row t of head h attends to, for the same scores.
All inputs are finite; a program needn't handle non-finite values.
Results may differ from the reference program's by a relative error of at most 0.013.
Values may be sent and summed in bfloat16 or wider, within the bound.
A program may use at most 192 MiB of HBM per device.

```python
import jax
import jax.numpy as jnp
from jax import lax

D = 8192
HD = 128
GROUP = 16
LEN = 1024
HEADS = 32
KV_HEADS = 2
TOKENS = 4096


def draw_inputs(key):
    key_query = jax.random.fold_in(key, 101)
    key_keys = jax.random.fold_in(key, 202)
    key_values = jax.random.fold_in(key, 303)
    query = jnp.clip(jax.random.normal(key_query, (TOKENS, HEADS * HD), jnp.float32), -6.0, 6.0)
    keys = jnp.clip(jax.random.normal(key_keys, (TOKENS, KV_HEADS * HD), jnp.float32), -6.0, 6.0)
    values = jnp.clip(jax.random.normal(key_values, (TOKENS, KV_HEADS * HD), jnp.float32), -6.0, 6.0)
    return (query.astype(jnp.bfloat16), keys.astype(jnp.bfloat16), values.astype(jnp.bfloat16))


def forward_pass(key):
    query, keys, values = draw_inputs(key)
    seq_count = TOKENS // LEN
    query_split = query.astype(jnp.float32).reshape(seq_count, LEN, KV_HEADS, GROUP, HD)
    query_split = query_split.transpose(0, 2, 3, 1, 4).reshape(seq_count * KV_HEADS, GROUP, LEN, HD)
    keys_split = keys.astype(jnp.float32).reshape(seq_count, LEN, KV_HEADS, HD)
    keys_split = keys_split.transpose(0, 2, 1, 3).reshape(seq_count * KV_HEADS, LEN, HD)
    values_split = values.astype(jnp.float32).reshape(seq_count, LEN, KV_HEADS, HD)
    values_split = values_split.transpose(0, 2, 1, 3).reshape(seq_count * KV_HEADS, LEN, HD)
    positions = jnp.arange(LEN, dtype=jnp.int32)
    causal = positions[:, None] >= positions[None, :]

    def single(inputs):
        query_group, key_one, value_one = inputs
        scores = jnp.einsum('gqd,kd->gqk', query_group, key_one) * HD ** (-0.5)
        masked = jnp.where(causal[None], scores, -1e+30)
        highest = jnp.max(masked, axis=2, keepdims=True)
        log_total = highest[:, :, 0] + jnp.log(jnp.sum(jnp.exp(masked - highest), axis=2))
        weights_soft = jnp.exp(masked - log_total[:, :, None])
        output = jnp.einsum('gqk,kd->gqd', weights_soft, value_one)
        return (output, log_total)
    outputs, log_totals = lax.map(single, (query_split, keys_split, values_split))
    attended = outputs.reshape(seq_count, KV_HEADS, GROUP, LEN, HD).transpose(0, 3, 1, 2, 4)
    attended = attended.reshape(TOKENS, HEADS * HD)
    stats = log_totals.reshape(seq_count, KV_HEADS, GROUP, LEN).transpose(1, 2, 0, 3).reshape(HEADS, TOKENS)
    return (attended, stats)


def draw_query(key, part):
    return draw_inputs(key)[0]


def draw_keys(key, part):
    return draw_inputs(key)[1]


def draw_values(key, part):
    return draw_inputs(key)[2]


def draw_attended(key, part):
    return forward_pass(key)[0].astype(jnp.bfloat16)


def draw_stats(key, part):
    return forward_pass(key)[1].astype(jnp.float32)


def spiked(drawn, rng, source, target, shards_of, factor):
    owner, partner = [(jnp.arange(drawn.shape[dim]) // (drawn.shape[dim] // shards_of)).reshape([-1 if axis == dim else 1 for axis in range(drawn.ndim)]) for dim in (source, target)]
    chosen = jax.random.permutation(rng, shards_of)[partner]
    strong = (owner == chosen) | (owner == (partner + shards_of // 2) % shards_of)
    return jnp.where(strong, factor * drawn, drawn)


def block_levels(rng, dims, split, low, high):
    factor_of = 1.0
    for dim, blocks in split:
        heights = jax.random.uniform(jax.random.fold_in(jax.random.fold_in(rng, 6), dim), (blocks,), jnp.float32, low / len(split), high / len(split))
        factor_of = factor_of * jnp.repeat(jnp.exp(heights), dims[dim] // blocks).reshape((-1,) + (1,) * (len(dims) - 1 - dim))
    return factor_of


def noise(rng, dims, width, reach, cuts=(), kind=jnp.bfloat16):
    loudness = block_levels(rng, dims, cuts, -0.22, 0.18) if cuts else 1.0
    entries = jax.random.normal(rng, dims, jnp.float32) * width * loudness
    return jnp.minimum(jnp.maximum(entries, -reach), reach).astype(kind)


def gaussian_with(own_key, extent, deviation, reach, cuts, heavy, kind=jnp.bfloat16):
    entries = deviation * jax.random.normal(own_key, extent, jnp.float32)
    if cuts:
        entries = entries * block_levels(own_key, extent, cuts, -0.22, 0.18)
    return jnp.clip(spiked(entries, jax.random.fold_in(own_key, 3), *heavy), -reach, reach).astype(kind)


def setup_inputs(seed: int = 0) -> dict:
    key_of = jax.random.split(jax.random.key(seed), 8)
    return {
        "grad_out": gaussian_with(key_of[0], (TOKENS, D), 1.0, 6.0, ((0, 32),), (0, 1, 32, 2.75)),
        "out_weight": noise(key_of[1], (D, HEADS * HD), D ** -0.5, 0.0625, ((0, 4), (1, 8))),
        "query": draw_query(jax.random.fold_in(key_of[7], 71), 0),
        "keys": draw_keys(jax.random.fold_in(key_of[7], 71), 0),
        "values": draw_values(jax.random.fold_in(key_of[7], 71), 0),
        "attended": draw_attended(jax.random.fold_in(key_of[7], 71), 0),
        "stats": draw_stats(jax.random.fold_in(key_of[7], 71), 0),
    }


def split_heads(array, seq_count):
    shaped = array.reshape(seq_count, LEN, KV_HEADS, GROUP, HD).transpose(0, 2, 3, 1, 4)
    return shaped.reshape(seq_count * KV_HEADS, GROUP, LEN, HD)

def join_heads(array, seq_count):
    shaped = array.reshape(seq_count, KV_HEADS, GROUP, LEN, HD).transpose(0, 3, 1, 2, 4)
    return shaped.reshape(seq_count * LEN, KV_HEADS * GROUP * HD)

def split_keys(array, seq_count):
    shaped = array.reshape(seq_count, LEN, KV_HEADS, HD).transpose(0, 2, 1, 3)
    return shaped.reshape(seq_count * KV_HEADS, LEN, HD)

def join_keys(array, seq_count):
    shaped = array.reshape(seq_count, KV_HEADS, LEN, HD).transpose(0, 2, 1, 3)
    return shaped.reshape(seq_count * LEN, KV_HEADS * HD)

def head_grads(inputs):
    query_group, key_one, value_one, attended_group, grad_group, stats_group = inputs
    score_scale = HD ** (-0.5)
    query_wide = query_group.astype(jnp.float32)
    key_wide = key_one.astype(jnp.float32)
    grad_wide = grad_group.astype(jnp.float32)
    positions = jnp.arange(LEN, dtype=jnp.int32)
    causal = positions[:, None] >= positions[None, :]
    scores = jnp.einsum('gqd,kd->gqk', query_wide, key_wide) * score_scale
    attention = jnp.where(causal[None], jnp.exp(scores - stats_group[:, :, None]), 0.0)
    attention_low = lax.optimization_barrier(attention.astype(jnp.bfloat16)).astype(jnp.float32)
    grad_attention = jnp.einsum('gqd,kd->gqk', grad_wide, value_one.astype(jnp.float32))
    row_offset = lax.optimization_barrier(jnp.sum(grad_wide * attended_group.astype(jnp.float32), axis=2))
    grad_scores = attention * (grad_attention - row_offset[:, :, None])
    grad_scores = lax.optimization_barrier(grad_scores.astype(jnp.bfloat16)).astype(jnp.float32)
    query_grad = (jnp.einsum('gqk,kd->gqd', grad_scores, key_wide) * score_scale).astype(jnp.bfloat16)
    key_grad = (jnp.einsum('gqk,gqd->kd', grad_scores, query_wide) * score_scale).astype(jnp.bfloat16)
    value_grad = jnp.einsum('gqk,gqd->kd', attention_low, grad_wide).astype(jnp.bfloat16)
    return (query_grad, key_grad, value_grad)

def reference(grad_out, out_weight, query, keys, values, attended, stats):
    seq_count = TOKENS // LEN
    grad_att = jnp.dot(grad_out, out_weight, preferred_element_type=jnp.float32).astype(jnp.bfloat16)
    grad_seqs = grad_out.reshape(seq_count, LEN, D)
    attended_seqs = attended.reshape(seq_count, LEN, HEADS * HD)

    def add_grad(running, pair):
        grad_block, attended_block = pair
        grad_term = lax.dot_general(grad_block, attended_block, (((0,), (0,)), ((), ())), preferred_element_type=jnp.float32)
        rounded = lax.optimization_barrier(grad_term.astype(jnp.bfloat16))
        return (running + rounded.astype(jnp.float32), None)
    weight_sum, _ = lax.scan(add_grad, jnp.zeros((D, HEADS * HD), jnp.float32), (grad_seqs, attended_seqs))
    weight_grad = weight_sum.astype(jnp.bfloat16)
    stats_split = stats.reshape(KV_HEADS, GROUP, seq_count, LEN).transpose(2, 0, 1, 3)
    stats_split = stats_split.reshape(seq_count * KV_HEADS, GROUP, LEN)
    query_parts, key_parts, value_parts = lax.map(head_grads, (split_heads(query, seq_count), split_keys(keys, seq_count), split_keys(values, seq_count), split_heads(attended, seq_count), split_heads(grad_att, seq_count), stats_split))
    query_grad = join_heads(query_parts, seq_count)
    key_grad = join_keys(key_parts, seq_count)
    value_grad = join_keys(value_parts, seq_count)
    return (query_grad, key_grad, value_grad, weight_grad)
```

```python
import functools

import jax
import jax.numpy as jnp
from jax import lax
from jax.experimental import pallas as pl
from jax.experimental.pallas import tpu as pltpu
from jax.sharding import PartitionSpec as P

HD = 128
GROUP = 16
CHUNKS = 4


def partner(value, axis, mask):
    pairs = [(source, source ^ mask) for source in range(lax.axis_size(axis))]
    return lax.ppermute(value, axis, pairs)


def nt_dot(a, b):
    return lax.dot_general(a, b, (((1,), (1,)), ((), ())), preferred_element_type=jnp.float32)


def attention_kernel(block, q_ref, k_ref, kt_ref, v_ref, o_ref, g_ref, s_ref, dq_ref, dk_ref, dv_ref):
    head = pl.program_id(0)
    length = q_ref.shape[0]
    scale = HD ** (-0.5)

    @pl.when(head == 0)
    def _():
        dk_ref[...] = jnp.zeros_like(dk_ref)
        dv_ref[...] = jnp.zeros_like(dv_ref)

    ones = jnp.ones((8, HD), jnp.float32)
    for j in range(length // block):
        rows = pl.ds(j * block, block)
        span = (j + 1) * block
        q = q_ref[rows, :]
        g = g_ref[rows, :]
        product = g.astype(jnp.float32) * o_ref[rows, :].astype(jnp.float32)
        offset = lax.dot_general(
            ones, product, (((1,), (1,)), ((), ())),
            preferred_element_type=jnp.float32, precision=lax.Precision.HIGHEST,
        )[:1, :]
        stat = s_ref[pl.ds(head, 1), rows]
        scores = nt_dot(k_ref[:span, :], q) * scale
        key_pos = lax.broadcasted_iota(jnp.int32, (span, block), 0)
        query_pos = lax.broadcasted_iota(jnp.int32, (span, block), 1) + j * block
        attention = jnp.where(key_pos <= query_pos, jnp.exp(scores - stat), 0.0)
        grad_attention = nt_dot(v_ref[:span, :], g)
        grad_scores = (attention * (grad_attention - offset)).astype(jnp.bfloat16)
        dv_ref[:span, :] += jnp.dot(
            attention.astype(jnp.bfloat16), g, preferred_element_type=jnp.float32
        )
        dk_ref[:span, :] += jnp.dot(grad_scores, q, preferred_element_type=jnp.float32)
        dq_t = jnp.dot(kt_ref[:, :span], grad_scores, preferred_element_type=jnp.float32)
        dq_ref[rows, :] = (dq_t * scale).T.astype(dq_ref.dtype)

    @pl.when(head == pl.num_programs(0) - 1)
    def _():
        dk_ref[...] = dk_ref[...] * scale


def attention_grads(query, key_one, value_one, attended, grad_att, stats):
    length, width = query.shape
    heads = width // HD
    per_head = pl.BlockSpec((length, HD), lambda h: (0, h))
    shared = pl.BlockSpec((length, HD), lambda h: (0, 0))
    return pl.pallas_call(
        functools.partial(attention_kernel, 256),
        grid=(heads,),
        in_specs=[
            per_head,
            shared,
            pl.BlockSpec((HD, length), lambda h: (0, 0)),
            shared,
            per_head,
            per_head,
            pl.BlockSpec((heads, length), lambda h: (0, 0)),
        ],
        out_specs=[per_head, shared, shared],
        out_shape=[
            jax.ShapeDtypeStruct((length, width), jnp.bfloat16),
            jax.ShapeDtypeStruct((length, HD), jnp.float32),
            jax.ShapeDtypeStruct((length, HD), jnp.float32),
        ],
        compiler_params=pltpu.CompilerParams(
            dimension_semantics=("arbitrary",), vmem_limit_bytes=40 * 2**20
        ),
        cost_estimate=pl.CostEstimate(
            flops=10 * heads * length * length * HD,
            bytes_accessed=10 * length * width,
            transcendentals=heads * length * length,
        ),
        name="attention_grads",
    )(query, key_one, key_one.T, value_one, attended, grad_att, stats)


def add_term(total, chunk, part, weights):
    own, w_x, w_y, w_lo, w_hi = weights
    half_rows = w_lo.shape[0]
    if part.stop <= half_rows:
        far = w_lo[part]
    else:
        far = w_hi[part.start - half_rows : part.stop - half_rows]
    weight = jnp.concatenate([own[part], w_x[part], w_y[part], far], axis=0)
    term = jnp.dot(chunk, weight, preferred_element_type=jnp.float32)
    return term if total is None else total + term


def projection_chunked(grad_out, out_weight, attended):
    dp = lax.axis_size("dp")
    me = lax.axis_index("dp")
    rows, depth = out_weight.shape[0], out_weight.shape[0] // CHUNKS
    half_rows, half_cols = rows // 2, out_weight.shape[1] // 2
    w_x = partner(out_weight, "dp", 1)
    w_y = partner(out_weight, "dp", 2)
    blocks = [lax.dynamic_slice_in_dim(grad_out, (me ^ r) * rows, rows, 1) for r in range(dp)]
    total = None
    parts = []
    owned = []
    for c in range(CHUNKS):
        part = slice(c * depth, (c + 1) * depth)
        mine = jnp.concatenate([b[:, part] for b in blocks], axis=1)
        if c >= 3:
            mine, owned[c - 3] = lax.optimization_barrier((mine, owned[c - 3]))
        chunk = lax.all_gather(mine, "tensor", axis=0, tiled=True)
        if c == 0:
            chunk, w_x, w_y = lax.optimization_barrier((chunk, w_x, w_y))
        elif c == 1:
            w_lo = partner(w_y[:half_rows], "dp", 1)
            w_hi = partner(w_x[half_rows:], "dp", 2)
            chunk, w_lo, w_hi = lax.optimization_barrier((chunk, w_lo, w_hi))
        else:
            chunk, total, owned[-1] = lax.optimization_barrier((chunk, total, owned[-1]))
        partial = lax.dot_general(
            chunk, attended, (((0,), (0,)), ((), ())), preferred_element_type=jnp.float32
        ).astype(jnp.bfloat16)
        chunk, partial = lax.optimization_barrier((chunk, partial))
        partial = partial.reshape(dp, depth, -1)
        left, right = partial[:, :, :half_cols], partial[:, :, half_cols:]
        send_left = jnp.stack([left[1], left[3]])
        send_right = jnp.stack([right[2], right[3]])
        parts.append((chunk, part))
        if c >= 1:
            for done, where in parts:
                total = add_term(total, done, where, (out_weight, w_x, w_y, w_lo, w_hi))
            parts = []
        if c == CHUNKS - 1:
            total, send_left, send_right = lax.optimization_barrier((total, send_left, send_right))
        got = partner(send_left, "dp", 1)
        keep = left[0].astype(jnp.float32) + got[0].astype(jnp.float32)
        pass_on = left[2].astype(jnp.float32) + got[1].astype(jnp.float32)
        out_left = keep + partner(pass_on.astype(jnp.bfloat16), "dp", 2).astype(jnp.float32)
        got = partner(send_right, "dp", 2)
        keep = right[0].astype(jnp.float32) + got[0].astype(jnp.float32)
        pass_on = right[1].astype(jnp.float32) + got[1].astype(jnp.float32)
        out_right = keep + partner(pass_on.astype(jnp.bfloat16), "dp", 1).astype(jnp.float32)
        owned.append(jnp.concatenate([out_left, out_right], axis=1).astype(jnp.bfloat16))
    return total.astype(jnp.bfloat16), jnp.concatenate(owned, axis=0)


def projection_plain(grad_out, out_weight, attended):
    grad_rows = lax.all_gather(grad_out, "tensor", axis=0, tiled=True)
    grad_att = jnp.dot(
        grad_rows,
        lax.all_gather(out_weight, "dp", axis=0, tiled=True),
        preferred_element_type=jnp.float32,
    ).astype(jnp.bfloat16)
    weight_grad = lax.psum_scatter(
        lax.dot_general(
            grad_rows, attended, (((0,), (0,)), ((), ())), preferred_element_type=jnp.float32
        ).astype(jnp.bfloat16),
        "dp",
        scatter_dimension=0,
        tiled=True,
    )
    return grad_att, weight_grad


def per_device(grad_out, out_weight, query, keys, values, attended, stats):
    heads = query.shape[1] // HD
    project = projection_chunked if lax.axis_size("dp") == 4 else projection_plain
    grad_att, weight_grad = project(grad_out, out_weight, attended)
    tensor_index = lax.axis_index("tensor")
    key_head = tensor_index * heads // GROUP
    key_one = lax.dynamic_slice_in_dim(keys, key_head * HD, HD, 1)
    value_one = lax.dynamic_slice_in_dim(values, key_head * HD, HD, 1)
    query_grad, key_part, value_part = attention_grads(
        query, key_one, value_one, attended, grad_att, stats
    )
    group_span = GROUP // heads
    group_place = tensor_index % group_span
    bit_count = group_span.bit_length() - 1
    running_kv = jnp.stack([key_part, value_part])
    for bit_number in reversed(range(bit_count)):
        half_cols = running_kv.shape[2] // 2
        lower_cols = running_kv[:, :, :half_cols]
        upper_cols = running_kv[:, :, half_cols:]
        upper_half = group_place // (1 << bit_number) % 2 == 1
        kept_cols = jnp.where(upper_half, upper_cols, lower_cols)
        sent_cols = jnp.where(upper_half, lower_cols, upper_cols)
        running_kv = kept_cols + partner(
            sent_cols.astype(jnp.bfloat16), "tensor", 1 << bit_number
        ).astype(sent_cols.dtype)
    key_grad = running_kv[0].astype(jnp.bfloat16)
    value_grad = running_kv[1].astype(jnp.bfloat16)
    return (query_grad, key_grad, value_grad, weight_grad)


def solution(mesh):
    placed = (
        P(("dp", "tensor"), None),
        P("dp", "tensor"),
        P("dp", "tensor"),
        P("dp", None),
        P("dp", None),
        P("dp", "tensor"),
        P("tensor", "dp"),
    )
    return jax.shard_map(
        per_device,
        mesh=mesh,
        in_specs=placed,
        out_specs=(P("dp", "tensor"), P("dp", "tensor"), P("dp", "tensor"), P("dp", "tensor")),
        check_vma=False,
    )
```

```python
import functools

import jax
import jax.numpy as jnp
from jax import lax
from jax.experimental import pallas as pl
from jax.experimental.pallas import tpu as pltpu
from jax.sharding import PartitionSpec as P


HD = 128
GROUP = 16
CHUNKS = 4


def partner(value, axis, mask):
    pairs = [(source, source ^ mask) for source in range(lax.axis_size(axis))]
    return lax.ppermute(value, axis, pairs)


def nt_dot(a, b):
    return lax.dot_general(a, b, (((1,), (1,)), ((), ())), preferred_element_type=jnp.float32)


def attention_kernel(block, q_ref, k_ref, kt_ref, v_ref, o_ref, g_ref, s_ref, dq_ref, dk_ref, dv_ref):
    head = pl.program_id(0)
    length = q_ref.shape[0]
    scale = HD ** (-0.5)

    @pl.when(head == 0)
    def _():
        dk_ref[...] = jnp.zeros_like(dk_ref)
        dv_ref[...] = jnp.zeros_like(dv_ref)

    ones = jnp.ones((8, HD), jnp.float32)
    for j in range(length // block):
        rows = pl.ds(j * block, block)
        span = (j + 1) * block
        q = q_ref[rows, :]
        g = g_ref[rows, :]
        product = g.astype(jnp.float32) * o_ref[rows, :].astype(jnp.float32)
        offset = lax.dot_general(
            ones, product, (((1,), (1,)), ((), ())),
            preferred_element_type=jnp.float32, precision=lax.Precision.HIGHEST,
        )[:1, :]
        stat = s_ref[pl.ds(head, 1), rows]
        scores = nt_dot(k_ref[:span, :], q) * scale
        key_pos = lax.broadcasted_iota(jnp.int32, (span, block), 0)
        query_pos = lax.broadcasted_iota(jnp.int32, (span, block), 1) + j * block
        attention = jnp.where(key_pos <= query_pos, jnp.exp(scores - stat), 0.0)
        grad_attention = nt_dot(v_ref[:span, :], g)
        grad_scores = (attention * (grad_attention - offset)).astype(jnp.bfloat16)
        dv_ref[:span, :] += jnp.dot(
            attention.astype(jnp.bfloat16), g, preferred_element_type=jnp.float32
        )
        dk_ref[:span, :] += jnp.dot(grad_scores, q, preferred_element_type=jnp.float32)
        dq_t = jnp.dot(kt_ref[:, :span], grad_scores, preferred_element_type=jnp.float32)
        dq_ref[rows, :] = (dq_t * scale).T.astype(dq_ref.dtype)

    @pl.when(head == pl.num_programs(0) - 1)
    def _():
        dk_ref[...] = dk_ref[...] * scale


def attention_grads(query, key_one, value_one, attended, grad_att, stats):
    length, width = query.shape
    heads = width // HD
    per_head = pl.BlockSpec((length, HD), lambda h: (0, h))
    shared = pl.BlockSpec((length, HD), lambda h: (0, 0))
    return pl.pallas_call(
        functools.partial(attention_kernel, 256),
        grid=(heads,),
        in_specs=[
            per_head,
            shared,
            pl.BlockSpec((HD, length), lambda h: (0, 0)),
            shared,
            per_head,
            per_head,
            pl.BlockSpec((heads, length), lambda h: (0, 0)),
        ],
        out_specs=[per_head, shared, shared],
        out_shape=[
            jax.ShapeDtypeStruct((length, width), jnp.bfloat16),
            jax.ShapeDtypeStruct((length, HD), jnp.float32),
            jax.ShapeDtypeStruct((length, HD), jnp.float32),
        ],
        compiler_params=pltpu.CompilerParams(
            dimension_semantics=("arbitrary",), vmem_limit_bytes=40 * 2**20
        ),
        cost_estimate=pl.CostEstimate(
            flops=10 * heads * length * length * HD,
            bytes_accessed=10 * length * width,
            transcendentals=heads * length * length,
        ),
        name="attention_grads",
    )(query, key_one, key_one.T, value_one, attended, grad_att, stats)


def add_term(total, chunk, part, weights):
    own, w_x, w_y, w_lo, w_hi = weights
    half_rows = w_lo.shape[0]
    if part.stop <= half_rows:
        far = w_lo[part]
    else:
        far = w_hi[part.start - half_rows : part.stop - half_rows]
    weight = jnp.concatenate([own[part], w_x[part], w_y[part], far], axis=0)
    term = jnp.dot(chunk, weight, preferred_element_type=jnp.float32)
    return term if total is None else total + term


def projection_chunked(grad_out, out_weight, attended):
    dp, tensor = lax.axis_size("dp"), lax.axis_size("tensor")
    me = lax.axis_index("dp")
    place = lax.axis_index("tensor")
    chips = tensor // 2
    ring = [(source, (source + 2) % tensor) for source in range(tensor)]
    local = grad_out.shape[0]
    rows, depth = out_weight.shape[0], out_weight.shape[0] // CHUNKS
    half_rows, half_depth = rows // 2, depth // 2
    w_x = partner(out_weight, "dp", 1)
    w_y = partner(out_weight, "dp", 2)
    order = []
    for k in range(chips):
        holder = (place + tensor - 2 * k) % tensor
        order += [holder, holder ^ 1]
    attended = jnp.concatenate(
        [lax.dynamic_slice_in_dim(attended, h * local, local, 0) for h in order], axis=0
    )
    total = None
    parts = []
    owned = []
    arrived = []
    for c in range(CHUNKS):
        mine = jnp.concatenate(
            [
                lax.dynamic_slice_in_dim(grad_out, (me ^ r) * rows + c * depth, depth, 1)
                for r in range(dp)
            ],
            axis=1,
        )
        if c >= 2:
            mine, arrived[c - 2][-2] = lax.optimization_barrier((mine, arrived[c - 2][-2]))
        slots = [mine]
        for _ in range(chips - 1):
            slots.append(lax.ppermute(slots[-1], "tensor", ring))
        arrived.append(slots)
    for c in range(CHUNKS):
        part = slice(c * depth, (c + 1) * depth)
        blocks = []
        for slot in arrived[c]:
            blocks += [slot, partner(slot, "tensor", 1)]
        if c == 0:
            blocks[0], w_x, w_y = lax.optimization_barrier((blocks[0], w_x, w_y))
        elif c == 1:
            w_lo = partner(w_y[:half_rows], "dp", 1)
            w_hi = partner(w_x[half_rows:], "dp", 2)
            blocks[0], w_lo, w_hi = lax.optimization_barrier((blocks[0], w_lo, w_hi))
        else:
            blocks[0], total, owned[-1] = lax.optimization_barrier((blocks[0], total, owned[-1]))
        chunk = jnp.concatenate(blocks, axis=0)
        partial = lax.dot_general(
            chunk, attended, (((0,), (0,)), ((), ())), preferred_element_type=jnp.float32
        ).astype(jnp.bfloat16)
        chunk, partial = lax.optimization_barrier((chunk, partial))
        partial = partial.reshape(dp, depth, -1)
        upper, lower = partial[:, :half_depth], partial[:, half_depth:]
        send_upper = jnp.stack([upper[1], upper[3]])
        send_lower = lower[2:4]
        parts.append((chunk, part))
        if c >= 1:
            for done, where in parts:
                total = add_term(total, done, where, (out_weight, w_x, w_y, w_lo, w_hi))
            parts = []
        if c == CHUNKS - 1:
            total, send_upper, send_lower = lax.optimization_barrier(
                (total, send_upper, send_lower)
            )
        got_upper = partner(send_upper, "dp", 1)
        got_lower = partner(send_lower, "dp", 2)
        keep = upper[0].astype(jnp.float32) + got_upper[0].astype(jnp.float32)
        pass_on = upper[2].astype(jnp.float32) + got_upper[1].astype(jnp.float32)
        out_upper = keep + partner(pass_on.astype(jnp.bfloat16), "dp", 2).astype(jnp.float32)
        keep = lower[0].astype(jnp.float32) + got_lower[0].astype(jnp.float32)
        pass_on = lower[1].astype(jnp.float32) + got_lower[1].astype(jnp.float32)
        out_lower = keep + partner(pass_on.astype(jnp.bfloat16), "dp", 1).astype(jnp.float32)
        owned.append(jnp.concatenate([out_upper, out_lower], axis=0).astype(jnp.bfloat16))
    grad_att = total.astype(jnp.bfloat16)
    unrolled = jnp.zeros_like(grad_att)
    for k, h in enumerate(order):
        unrolled = lax.dynamic_update_slice_in_dim(
            unrolled, grad_att[k * local : (k + 1) * local], h * local, 0
        )
    return unrolled, jnp.concatenate(owned, axis=0)


def projection_plain(grad_out, out_weight, attended):
    grad_rows = lax.all_gather(grad_out, "tensor", axis=0, tiled=True)
    grad_att = jnp.dot(
        grad_rows,
        lax.all_gather(out_weight, "dp", axis=0, tiled=True),
        preferred_element_type=jnp.float32,
    ).astype(jnp.bfloat16)
    weight_grad = lax.psum_scatter(
        lax.dot_general(
            grad_rows, attended, (((0,), (0,)), ((), ())), preferred_element_type=jnp.float32
        ).astype(jnp.bfloat16),
        "dp",
        scatter_dimension=0,
        tiled=True,
    )
    return grad_att, weight_grad


def per_device(grad_out, out_weight, query, keys, values, attended, stats):
    heads = query.shape[1] // HD
    project = projection_chunked if lax.axis_size("dp") == 4 else projection_plain
    grad_att, weight_grad = project(grad_out, out_weight, attended)
    tensor_index = lax.axis_index("tensor")
    key_head = tensor_index * heads // GROUP
    key_one = lax.dynamic_slice_in_dim(keys, key_head * HD, HD, 1)
    value_one = lax.dynamic_slice_in_dim(values, key_head * HD, HD, 1)
    query_grad, key_part, value_part = attention_grads(
        query, key_one, value_one, attended, grad_att, stats
    )
    group_span = GROUP // heads
    group_place = tensor_index % group_span
    bit_count = group_span.bit_length() - 1
    running_kv = jnp.stack([key_part, value_part])
    for bit_number in reversed(range(bit_count)):
        half_cols = running_kv.shape[2] // 2
        lower_cols = running_kv[:, :, :half_cols]
        upper_cols = running_kv[:, :, half_cols:]
        upper_half = group_place // (1 << bit_number) % 2 == 1
        kept_cols = jnp.where(upper_half, upper_cols, lower_cols)
        sent_cols = jnp.where(upper_half, lower_cols, upper_cols)
        running_kv = kept_cols + partner(
            sent_cols.astype(jnp.bfloat16), "tensor", 1 << bit_number
        ).astype(sent_cols.dtype)
    key_grad = running_kv[0].astype(jnp.bfloat16)
    value_grad = running_kv[1].astype(jnp.bfloat16)
    return (query_grad, key_grad, value_grad, weight_grad)


def solution(mesh):
    placed = (
        P(("dp", "tensor"), None),
        P("dp", "tensor"),
        P("dp", "tensor"),
        P("dp", None),
        P("dp", None),
        P("dp", "tensor"),
        P("tensor", "dp"),
    )
    return jax.shard_map(
        per_device,
        mesh=mesh,
        in_specs=placed,
        out_specs=(P("dp", "tensor"), P("dp", "tensor"), P("dp", "tensor"), P("dp", "tensor")),
        check_vma=False,
    )
```

```python
import functools

import jax
import jax.numpy as jnp
from jax import lax
from jax.experimental import pallas as pl
from jax.experimental.pallas import tpu as pltpu
from jax.sharding import PartitionSpec as P


HD = 128
GROUP = 16
CHUNKS = 4


def partner(value, axis, mask):
    pairs = [(source, source ^ mask) for source in range(lax.axis_size(axis))]
    return lax.ppermute(value, axis, pairs)


def nt_dot(a, b):
    return lax.dot_general(a, b, (((1,), (1,)), ((), ())), preferred_element_type=jnp.float32)


def attention_kernel(block, q_ref, k_ref, kt_ref, v_ref, o_ref, g_ref, s_ref, dq_ref, dkt_ref, dvt_ref, dk_ref, dv_ref):
    head = pl.program_id(0)
    length = q_ref.shape[0]
    scale = HD ** (-0.5)

    @pl.when(head == 0)
    def _():
        dk_ref[...] = jnp.zeros_like(dk_ref)
        dv_ref[...] = jnp.zeros_like(dv_ref)

    ones = jnp.ones((8, HD), jnp.float32)
    for j in range(length // block):
        rows = pl.ds(j * block, block)
        span = (j + 1) * block
        q = q_ref[rows, :]
        g = g_ref[rows, :]
        product = g.astype(jnp.float32) * o_ref[rows, :].astype(jnp.float32)
        offset = lax.dot_general(
            ones, product, (((1,), (1,)), ((), ())),
            preferred_element_type=jnp.float32, precision=lax.Precision.HIGHEST,
        )[:1, :]
        stat = s_ref[pl.ds(head, 1), rows]
        scores = nt_dot(k_ref[:span, :], q) * scale
        key_pos = lax.broadcasted_iota(jnp.int32, (span, block), 0)
        query_pos = lax.broadcasted_iota(jnp.int32, (span, block), 1) + j * block
        attention = jnp.where(key_pos <= query_pos, jnp.exp(scores - stat), 0.0)
        grad_attention = nt_dot(v_ref[:span, :], g)
        grad_scores = (attention * (grad_attention - offset)).astype(jnp.bfloat16)
        dv_ref[:span, :] += jnp.dot(
            attention.astype(jnp.bfloat16), g, preferred_element_type=jnp.float32
        )
        dk_ref[:span, :] += jnp.dot(grad_scores, q, preferred_element_type=jnp.float32)
        dq_t = jnp.dot(kt_ref[:, :span], grad_scores, preferred_element_type=jnp.float32)
        dq_ref[rows, :] = (dq_t * scale).T.astype(dq_ref.dtype)

    @pl.when(head == pl.num_programs(0) - 1)
    def _():
        dkt_ref[...] = (dk_ref[...] * scale).T
        dvt_ref[...] = dv_ref[...].T


def attention_grads(query, key_one, value_one, attended, grad_att, stats):
    length, width = query.shape
    heads = width // HD
    per_head = pl.BlockSpec((length, HD), lambda h: (0, h))
    shared = pl.BlockSpec((length, HD), lambda h: (0, 0))
    flat = pl.BlockSpec((HD, length), lambda h: (0, 0))
    return pl.pallas_call(
        functools.partial(attention_kernel, 256),
        grid=(heads,),
        in_specs=[
            per_head,
            shared,
            flat,
            shared,
            per_head,
            per_head,
            pl.BlockSpec((heads, length), lambda h: (0, 0)),
        ],
        out_specs=[per_head, flat, flat],
        scratch_shapes=[pltpu.VMEM((length, HD), jnp.float32)] * 2,
        out_shape=[
            jax.ShapeDtypeStruct((length, width), jnp.bfloat16),
            jax.ShapeDtypeStruct((HD, length), jnp.float32),
            jax.ShapeDtypeStruct((HD, length), jnp.float32),
        ],
        compiler_params=pltpu.CompilerParams(
            dimension_semantics=("arbitrary",), vmem_limit_bytes=40 * 2**20
        ),
        cost_estimate=pl.CostEstimate(
            flops=10 * heads * length * length * HD,
            bytes_accessed=10 * length * width,
            transcendentals=heads * length * length,
        ),
        name="attention_grads",
    )(query, key_one, key_one.T, value_one, attended, grad_att, stats)


def add_term(total, chunk, part, weights):
    own, w_x, w_y, w_lo, w_hi = weights
    half_rows = w_lo.shape[0]
    if part.stop <= half_rows:
        far = w_lo[part]
    else:
        far = w_hi[part.start - half_rows : part.stop - half_rows]
    weight = jnp.concatenate([own[part], w_x[part], w_y[part], far], axis=0)
    term = jnp.dot(chunk, weight, preferred_element_type=jnp.float32)
    return term if total is None else total + term


def projection_chunked(grad_out, out_weight, attended):
    dp, tensor = lax.axis_size("dp"), lax.axis_size("tensor")
    me = lax.axis_index("dp")
    place = lax.axis_index("tensor")
    chips = tensor // 2
    ring = [(source, (source + 2) % tensor) for source in range(tensor)]
    local = grad_out.shape[0]
    rows, depth = out_weight.shape[0], out_weight.shape[0] // CHUNKS
    half_rows, half_depth = rows // 2, depth // 2
    w_x = partner(out_weight, "dp", 1)
    w_y = partner(out_weight, "dp", 2)
    order = []
    for k in range(chips):
        holder = (place + tensor - 2 * k) % tensor
        order += [holder, holder ^ 1]
    attended = jnp.concatenate(
        [lax.dynamic_slice_in_dim(attended, h * local, local, 0) for h in order], axis=0
    )
    barrier = lax.optimization_barrier

    def cut(c):
        return jnp.concatenate(
            [
                lax.dynamic_slice_in_dim(grad_out, (me ^ r) * rows + c * depth, depth, 1)
                for r in range(dp)
            ],
            axis=1,
        )

    def hop(slot):
        return lax.ppermute(slot, "tensor", ring)

    def weight_term(chunk):
        return lax.dot_general(
            chunk, attended, (((0,), (0,)), ((), ())), preferred_element_type=jnp.float32
        ).astype(jnp.bfloat16)

    def joined(slots, tie=()):
        blocks = []
        for slot in slots:
            blocks += [slot, partner(slot, "tensor", 1)]
        blocks[0], *tie = barrier((blocks[0], *tie))
        return jnp.concatenate(blocks, axis=0), tie

    def sends(partial):
        partial = partial.reshape(dp, depth, -1)
        upper, lower = partial[:, :half_depth], partial[:, half_depth:]
        return upper, lower, jnp.stack([upper[1], upper[3]]), lower[2:4]

    def first(upper, lower):
        got_upper = partner(upper, "dp", 1)
        got_lower = partner(lower, "dp", 2)
        return got_upper, got_lower

    def second(upper, lower, got_upper, got_lower):
        wide = jnp.float32
        up = (upper[2].astype(wide) + got_upper[1].astype(wide)).astype(jnp.bfloat16)
        low = (lower[1].astype(wide) + got_lower[1].astype(wide)).astype(jnp.bfloat16)
        up = partner(up, "dp", 2)
        low = partner(low, "dp", 1)
        up = upper[0].astype(wide) + got_upper[0].astype(wide) + up.astype(wide)
        low = lower[0].astype(wide) + got_lower[0].astype(wide) + low.astype(wide)
        return jnp.concatenate([up, low], axis=0).astype(jnp.bfloat16)

    part = [slice(c * depth, (c + 1) * depth) for c in range(CHUNKS)]
    owned = []
    total = None
    late = None
    for pair in range(0, CHUNKS, 2):
        one, two = [cut(pair)], [cut(pair + 1)]
        if late is not None:
            one[0], late[0][-1] = barrier((one[0], late[0][-1]))
            two[0], late[1][-1] = barrier((two[0], late[1][-1]))
            chunk_0, (w_lo, w_hi) = joined(late[0], (w_lo, w_hi))
            partial = weight_term(chunk_0)
            chunk_0, partial = barrier((chunk_0, partial))
            upper, lower, *out = sends(partial)
            owned.append(second(upper, lower, *first(*out)))
            chunk_1, _ = joined(late[1])
            partial = weight_term(chunk_1)
            chunk_1, partial = barrier((chunk_1, partial))
            upper, lower, *out = sends(partial)
            owned.append(second(upper, lower, *first(*out)))
            weights = (out_weight, w_x, w_y, w_lo, w_hi)
            total = add_term(total, chunk_0, part[pair - 2], weights)
            total = add_term(total, chunk_1, part[pair - 1], weights)
        for step in range(1, chips):
            if late is not None and step == 2:
                one[-1], owned[-2] = barrier((one[-1], owned[-2]))
            if late is not None and step == 3:
                one[-1], owned[-1] = barrier((one[-1], owned[-1]))
                two[-1], total = barrier((two[-1], total))
            if late is None and step == chips - 1:
                two[-1], w_x, w_y = barrier((two[-1], w_x, w_y))
                w_lo = partner(w_y[:half_rows], "dp", 1)
                w_hi = partner(w_x[half_rows:], "dp", 2)
            one.append(hop(one[-1]))
            two.append(hop(two[-1]))
        late = (one, two)
    chunk_0, _ = joined(late[0])
    partial = weight_term(chunk_0)
    chunk_0, partial = barrier((chunk_0, partial))
    upper, lower, *out = sends(partial)
    got = first(*out)
    total = add_term(total, chunk_0, part[-2], weights)
    chunk_1, (total,) = joined(late[1], (total,))
    partial = weight_term(chunk_1)
    chunk_1, partial, *got = barrier((chunk_1, partial, *got))
    owned.append(second(upper, lower, *got))
    upper, lower, *out = sends(partial)
    owned.append(second(upper, lower, *first(*out)))
    total = add_term(total, chunk_1, part[-1], weights)
    grad_att = total.astype(jnp.bfloat16)
    unrolled = jnp.zeros_like(grad_att)
    for k, h in enumerate(order):
        unrolled = lax.dynamic_update_slice_in_dim(
            unrolled, grad_att[k * local : (k + 1) * local], h * local, 0
        )
    return unrolled, jnp.concatenate(owned, axis=0)


def projection_plain(grad_out, out_weight, attended):
    grad_rows = lax.all_gather(grad_out, "tensor", axis=0, tiled=True)
    grad_att = jnp.dot(
        grad_rows,
        lax.all_gather(out_weight, "dp", axis=0, tiled=True),
        preferred_element_type=jnp.float32,
    ).astype(jnp.bfloat16)
    weight_grad = lax.psum_scatter(
        lax.dot_general(
            grad_rows, attended, (((0,), (0,)), ((), ())), preferred_element_type=jnp.float32
        ).astype(jnp.bfloat16),
        "dp",
        scatter_dimension=0,
        tiled=True,
    )
    return grad_att, weight_grad


def per_device(grad_out, out_weight, query, keys, values, attended, stats):
    heads = query.shape[1] // HD
    project = projection_chunked if lax.axis_size("dp") == 4 else projection_plain
    grad_att, weight_grad = project(grad_out, out_weight, attended)
    tensor_index = lax.axis_index("tensor")
    key_head = tensor_index * heads // GROUP
    key_one = lax.dynamic_slice_in_dim(keys, key_head * HD, HD, 1)
    value_one = lax.dynamic_slice_in_dim(values, key_head * HD, HD, 1)
    query_grad, key_part, value_part = attention_grads(
        query, key_one, value_one, attended, grad_att, stats
    )
    group_span = GROUP // heads
    group_place = tensor_index % group_span
    width, length = HD // group_span, query.shape[0]
    running_kv = jnp.stack([key_part, value_part]).reshape(2, group_span, width, length)
    for bit_number in range(group_span.bit_length() - 1):
        pairs = running_kv.reshape(2, -1, 2, width, length)
        odd = (group_place >> bit_number) % 2 == 1
        kept = jnp.where(odd, pairs[:, :, 1], pairs[:, :, 0])
        sent = jnp.where(odd, pairs[:, :, 0], pairs[:, :, 1])
        running_kv = kept + partner(
            sent.astype(jnp.bfloat16), "tensor", 1 << bit_number
        ).astype(sent.dtype)
    key_grad = running_kv[0, 0].T.astype(jnp.bfloat16)
    value_grad = running_kv[1, 0].T.astype(jnp.bfloat16)
    return (query_grad, key_grad, value_grad, weight_grad)


def solution(mesh):
    placed = (
        P(("dp", "tensor"), None),
        P("dp", "tensor"),
        P("dp", "tensor"),
        P("dp", None),
        P("dp", None),
        P("dp", "tensor"),
        P("tensor", "dp"),
    )
    return jax.shard_map(
        per_device,
        mesh=mesh,
        in_specs=placed,
        out_specs=(P("dp", "tensor"), P("dp", "tensor"), P("dp", "tensor"), P("dp", "tensor")),
        check_vma=False,
    )
```

```python
import functools

import jax
import jax.numpy as jnp
from jax import lax
from jax.experimental import pallas as pl
from jax.experimental.pallas import tpu as pltpu
from jax.sharding import PartitionSpec as P


HD = 128
GROUP = 16
CHUNKS = 4


def partner(value, axis, mask):
    pairs = [(source, source ^ mask) for source in range(lax.axis_size(axis))]
    return lax.ppermute(value, axis, pairs)


def nt_dot(a, b):
    return lax.dot_general(a, b, (((1,), (1,)), ((), ())), preferred_element_type=jnp.float32)


def attention_kernel(block, q_ref, k_ref, kt_ref, v_ref, o_ref, g_ref, s_ref, dq_ref, dkt_ref, dvt_ref, dk_ref, dv_ref):
    head = pl.program_id(0)
    length = q_ref.shape[0]
    scale = HD ** (-0.5)

    @pl.when(head == 0)
    def _():
        dk_ref[...] = jnp.zeros_like(dk_ref)
        dv_ref[...] = jnp.zeros_like(dv_ref)

    ones = jnp.ones((8, HD), jnp.float32)
    for j in range(length // block):
        rows = pl.ds(j * block, block)
        span = (j + 1) * block
        q = q_ref[rows, :]
        g = g_ref[rows, :]
        product = g.astype(jnp.float32) * o_ref[rows, :].astype(jnp.float32)
        offset = lax.dot_general(
            ones, product, (((1,), (1,)), ((), ())),
            preferred_element_type=jnp.float32, precision=lax.Precision.HIGHEST,
        )[:1, :]
        stat = s_ref[pl.ds(head, 1), rows]
        scores = nt_dot(k_ref[:span, :], q) * scale
        key_pos = lax.broadcasted_iota(jnp.int32, (span, block), 0)
        query_pos = lax.broadcasted_iota(jnp.int32, (span, block), 1) + j * block
        attention = jnp.where(key_pos <= query_pos, jnp.exp(scores - stat), 0.0)
        grad_attention = nt_dot(v_ref[:span, :], g)
        grad_scores = (attention * (grad_attention - offset)).astype(jnp.bfloat16)
        dv_ref[:span, :] += jnp.dot(
            attention.astype(jnp.bfloat16), g, preferred_element_type=jnp.float32
        )
        dk_ref[:span, :] += jnp.dot(grad_scores, q, preferred_element_type=jnp.float32)
        dq_t = jnp.dot(kt_ref[:, :span], grad_scores, preferred_element_type=jnp.float32)
        dq_ref[rows, :] = (dq_t * scale).T.astype(dq_ref.dtype)

    @pl.when(head == pl.num_programs(0) - 1)
    def _():
        dkt_ref[...] = (dk_ref[...] * scale).T
        dvt_ref[...] = dv_ref[...].T


def attention_grads(query, key_one, value_one, attended, grad_att, stats):
    length, width = query.shape
    heads = width // HD
    per_head = pl.BlockSpec((length, HD), lambda h: (0, h))
    shared = pl.BlockSpec((length, HD), lambda h: (0, 0))
    flat = pl.BlockSpec((HD, length), lambda h: (0, 0))
    return pl.pallas_call(
        functools.partial(attention_kernel, 256),
        grid=(heads,),
        in_specs=[
            per_head,
            shared,
            flat,
            shared,
            per_head,
            per_head,
            pl.BlockSpec((heads, length), lambda h: (0, 0)),
        ],
        out_specs=[per_head, flat, flat],
        scratch_shapes=[pltpu.VMEM((length, HD), jnp.float32)] * 2,
        out_shape=[
            jax.ShapeDtypeStruct((length, width), jnp.bfloat16),
            jax.ShapeDtypeStruct((HD, length), jnp.float32),
            jax.ShapeDtypeStruct((HD, length), jnp.float32),
        ],
        compiler_params=pltpu.CompilerParams(
            dimension_semantics=("arbitrary",), vmem_limit_bytes=40 * 2**20
        ),
        cost_estimate=pl.CostEstimate(
            flops=10 * heads * length * length * HD,
            bytes_accessed=10 * length * width,
            transcendentals=heads * length * length,
        ),
        name="attention_grads",
    )(query, key_one, key_one.T, value_one, attended, grad_att, stats)


def add_term(total, chunk, part, weights):
    own, w_x, w_y, w_lo, w_hi = weights
    half_rows = w_lo.shape[0]
    if part.stop <= half_rows:
        far = w_lo[part]
    else:
        far = w_hi[part.start - half_rows : part.stop - half_rows]
    weight = jnp.concatenate([own[part], w_x[part], w_y[part], far], axis=0)
    term = jnp.dot(chunk, weight, preferred_element_type=jnp.float32)
    return term if total is None else total + term


def projection_chunked(grad_out, out_weight, attended):
    dp, tensor = lax.axis_size("dp"), lax.axis_size("tensor")
    me = lax.axis_index("dp")
    place = lax.axis_index("tensor")
    chips = tensor // 2
    ring = [(source, (source + 2) % tensor) for source in range(tensor)]
    local = grad_out.shape[0]
    rows, depth = out_weight.shape[0], out_weight.shape[0] // CHUNKS
    half_rows, half_depth = rows // 2, depth // 2
    w_x = partner(out_weight, "dp", 1)
    w_y = partner(out_weight, "dp", 2)
    order = []
    for k in range(chips):
        holder = (place + tensor - 2 * k) % tensor
        order += [holder, holder ^ 1]
    attended = jnp.concatenate(
        [lax.dynamic_slice_in_dim(attended, h * local, local, 0) for h in order], axis=0
    )
    barrier = lax.optimization_barrier

    def cut(c):
        return jnp.concatenate(
            [
                lax.dynamic_slice_in_dim(grad_out, (me ^ r) * rows + c * depth, depth, 1)
                for r in range(dp)
            ],
            axis=1,
        )

    def hop(slot):
        return lax.ppermute(slot, "tensor", ring)

    def weight_term(chunk):
        return lax.dot_general(
            chunk, attended, (((0,), (0,)), ((), ())), preferred_element_type=jnp.float32
        ).astype(jnp.bfloat16)

    def joined(slots, tie=()):
        blocks = []
        for slot in slots:
            blocks += [slot, partner(slot, "tensor", 1)]
        blocks[0], *tie = barrier((blocks[0], *tie))
        return jnp.concatenate(blocks, axis=0), tie

    def sends(partial):
        partial = partial.reshape(dp, depth, -1)
        upper, lower = partial[:, :half_depth], partial[:, half_depth:]
        return upper, lower, jnp.stack([upper[1], upper[3]]), lower[2:4]

    def first(upper, lower):
        got_upper = partner(upper, "dp", 1)
        got_lower = partner(lower, "dp", 2)
        return got_upper, got_lower

    def second(upper, lower, got_upper, got_lower):
        wide = jnp.float32
        up = (upper[2].astype(wide) + got_upper[1].astype(wide)).astype(jnp.bfloat16)
        low = (lower[1].astype(wide) + got_lower[1].astype(wide)).astype(jnp.bfloat16)
        up = partner(up, "dp", 2)
        low = partner(low, "dp", 1)
        up = upper[0].astype(wide) + got_upper[0].astype(wide) + up.astype(wide)
        low = lower[0].astype(wide) + got_lower[0].astype(wide) + low.astype(wide)
        return jnp.concatenate([up, low], axis=0).astype(jnp.bfloat16)

    part = [slice(c * depth, (c + 1) * depth) for c in range(CHUNKS)]
    owned = []
    total = None
    late = None
    for pair in range(0, CHUNKS, 2):
        one, two = [cut(pair)], [cut(pair + 1)]
        if late is not None:
            one[0], late[0][-1] = barrier((one[0], late[0][-1]))
            two[0], late[1][-1] = barrier((two[0], late[1][-1]))
            chunk_0, _ = joined(late[0])
            partial = weight_term(chunk_0)
            chunk_0, partial = barrier((chunk_0, partial))
            upper, lower, *out = sends(partial)
            owned.append(second(upper, lower, *first(*out)))
            chunk_1, (w_lo, w_hi) = joined(late[1], (w_lo, w_hi))
            partial = weight_term(chunk_1)
            chunk_1, partial = barrier((chunk_1, partial))
            upper, lower, *out = sends(partial)
            owned.append(second(upper, lower, *first(*out)))
            weights = (out_weight, w_x, w_y, w_lo, w_hi)
            total = add_term(total, chunk_0, part[pair - 2], weights)
            total = add_term(total, chunk_1, part[pair - 1], weights)
        for step in range(1, chips):
            if late is not None and step == chips - 1:
                one[-1], owned[-2] = barrier((one[-1], owned[-2]))
                two[-1], total, owned[-1] = barrier((two[-1], total, owned[-1]))
            if late is None and step == chips - 1:
                two[-1], w_x, w_y = barrier((two[-1], w_x, w_y))
                w_lo = partner(w_y[:half_rows], "dp", 1)
                w_hi = partner(w_x[half_rows:], "dp", 2)
            one.append(hop(one[-1]))
            two.append(hop(two[-1]))
        late = (one, two)
    chunk_0, _ = joined(late[0])
    partial = weight_term(chunk_0)
    chunk_0, partial = barrier((chunk_0, partial))
    upper, lower, *out = sends(partial)
    got = first(*out)
    total = add_term(total, chunk_0, part[-2], weights)
    chunk_1, (total,) = joined(late[1], (total,))
    partial = weight_term(chunk_1)
    chunk_1, partial = barrier((chunk_1, partial))
    owned.append(second(upper, lower, *got))
    upper, lower, *out = sends(partial)
    owned.append(second(upper, lower, *first(*out)))
    total = add_term(total, chunk_1, part[-1], weights)
    grad_att = total.astype(jnp.bfloat16)
    unrolled = jnp.zeros_like(grad_att)
    for k, h in enumerate(order):
        unrolled = lax.dynamic_update_slice_in_dim(
            unrolled, grad_att[k * local : (k + 1) * local], h * local, 0
        )
    return unrolled, jnp.concatenate(owned, axis=0)


def projection_plain(grad_out, out_weight, attended):
    grad_rows = lax.all_gather(grad_out, "tensor", axis=0, tiled=True)
    grad_att = jnp.dot(
        grad_rows,
        lax.all_gather(out_weight, "dp", axis=0, tiled=True),
        preferred_element_type=jnp.float32,
    ).astype(jnp.bfloat16)
    weight_grad = lax.psum_scatter(
        lax.dot_general(
            grad_rows, attended, (((0,), (0,)), ((), ())), preferred_element_type=jnp.float32
        ).astype(jnp.bfloat16),
        "dp",
        scatter_dimension=0,
        tiled=True,
    )
    return grad_att, weight_grad


def per_device(grad_out, out_weight, query, keys, values, attended, stats):
    heads = query.shape[1] // HD
    project = projection_chunked if lax.axis_size("dp") == 4 else projection_plain
    grad_att, weight_grad = project(grad_out, out_weight, attended)
    tensor_index = lax.axis_index("tensor")
    key_head = tensor_index * heads // GROUP
    key_one = lax.dynamic_slice_in_dim(keys, key_head * HD, HD, 1)
    value_one = lax.dynamic_slice_in_dim(values, key_head * HD, HD, 1)
    query_grad, key_part, value_part = attention_grads(
        query, key_one, value_one, attended, grad_att, stats
    )
    group_span = GROUP // heads
    group_place = tensor_index % group_span
    width, length = HD // group_span, query.shape[0]
    running_kv = jnp.stack([key_part, value_part]).reshape(2, group_span, width, length)
    for bit_number in range(group_span.bit_length() - 1):
        pairs = running_kv.reshape(2, -1, 2, width, length)
        odd = (group_place >> bit_number) % 2 == 1
        kept = jnp.where(odd, pairs[:, :, 1], pairs[:, :, 0])
        sent = jnp.where(odd, pairs[:, :, 0], pairs[:, :, 1])
        running_kv = kept + partner(
            sent.astype(jnp.bfloat16), "tensor", 1 << bit_number
        ).astype(sent.dtype)
    key_grad = running_kv[0, 0].T.astype(jnp.bfloat16)
    value_grad = running_kv[1, 0].T.astype(jnp.bfloat16)
    return (query_grad, key_grad, value_grad, weight_grad)


def solution(mesh):
    placed = (
        P(("dp", "tensor"), None),
        P("dp", "tensor"),
        P("dp", "tensor"),
        P("dp", None),
        P("dp", None),
        P("dp", "tensor"),
        P("tensor", "dp"),
    )
    return jax.shard_map(
        per_device,
        mesh=mesh,
        in_specs=placed,
        out_specs=(P("dp", "tensor"), P("dp", "tensor"), P("dp", "tensor"), P("dp", "tensor")),
        check_vma=False,
    )
```
